128 devices in a mesh: dp: 8 (over x, y_lo), vocab: 16 (over z, y_hi, core).
Axes of the slice: x: 4, y: 4 (y_hi: 2, y_lo: 2; y = y_hi * 2 + y_lo), z: 4, core: 2. Of those that a mesh axis runs over, the one named last changes fastest.
Arguments:
- hidden: bfloat16 [8192, 5120], P(('dp', 'vocab')), may hold values from -100 to 100
- tokens: int32 [8192], P('dp'), may hold values from 0 to 18431
- old_weight: bfloat16 [18432, 5120], P('vocab'), may hold values from -1 to 1
- new_weight: bfloat16 [18432, 5120], P('dp', 'vocab'), may hold values from -6 to 6
Outputs:
- logprob: float32 [8192], P(('dp', 'vocab'))
- engine_weight: bfloat16 [18432, 5120], P('vocab')
The draws below stay inside these ranges and needn't reach their ends.
All inputs are finite; a program needn't handle non-finite values.
Results may differ from the reference program's by a relative error of at most 0.001.
Values may be sent and summed in bfloat16 or wider, within the bound.
A program may use at most 128 MiB of HBM per device.

```python
import math
import jax
import jax.numpy as jnp
from jax import lax

D = 5120
VOCAB = 18432
GROUP_ROWS = 1024
ROWS = 8192
N_DP = 8


def base_weight(key):
    first_key = jax.random.fold_in(jax.random.fold_in(key, 11), 0)
    weights = jax.random.normal(first_key, (VOCAB, D), jnp.float32) / math.sqrt(D)
    return jnp.clip(weights, -1.0, 1.0)


def draw_old_weight(key, part):
    return base_weight(key).astype(jnp.bfloat16)


def draw_hidden(key, part):
    keys = jax.random.split(jax.random.fold_in(key, 23), 1)
    values = 3.0 * jax.random.normal(keys[0], (ROWS, D), jnp.float32)
    return jnp.clip(values, -100.0, 100.0).astype(jnp.bfloat16)


def set_ends(array, own_key, smallest, high):
    spot = [jax.random.randint(jax.random.fold_in(own_key, axis), (), 0, length) for axis, length in enumerate(array.shape)]
    longest = array.shape.index(max(array.shape))
    neighbour = spot[:longest] + [(spot[longest] + 1) % array.shape[longest]] + spot[longest + 1:]
    return array.at[tuple(spot)].set(smallest).at[tuple(neighbour)].set(high)


def levels(stream_key, shape, shards, least, top_value):
    gain = 1.0
    for position, shards_of in shards:
        steps = jax.random.uniform(jax.random.fold_in(jax.random.fold_in(stream_key, 6), position), (shards_of,), jnp.float32, least / len(shards), top_value / len(shards))
        gain = gain * jnp.repeat(jnp.exp(steps), shape[position] // shards_of).reshape((-1,) + (1,) * (len(shape) - 1 - position))
    return gain


def bell_draw(key, shape, deviation, bound, shards=(), dtype=jnp.bfloat16):
    result = deviation * jax.random.normal(key, shape, jnp.float32)
    if shards:
        result = result * levels(key, shape, shards, -0.22, 0.18)
    return jnp.clip(result, -bound, bound).astype(dtype)


def setup_inputs(seed: int = 0) -> dict:
    key_of = jax.random.split(jax.random.key(seed), 5)
    hidden = draw_hidden(jax.random.fold_in(key_of[4], 71), 0)
    tokens = set_ends(jax.random.randint(key_of[1], (ROWS,), 0, VOCAB), jax.random.fold_in(key_of[1], 1), 0, VOCAB - 1).astype(jnp.int32)
    old_weight = draw_old_weight(jax.random.fold_in(key_of[4], 71), 0)
    new_weight = bell_draw(key_of[3], (VOCAB, D), 1.0, 6.0, ((0, 8), (1, 16)))
    return dict(hidden=hidden, tokens=tokens, old_weight=old_weight, new_weight=new_weight)


def reference(hidden, tokens, old_weight, new_weight):
    def one_group(operands):
        rows, ids = operands
        logits = jnp.dot(rows, old_weight.T, preferred_element_type=jnp.float32)
        top = jnp.max(logits, axis=1)
        total = jnp.sum(jnp.exp(logits - top[:, None]), axis=1)
        target = jnp.take_along_axis(logits, ids[:, None].astype(jnp.int32), axis=1)[:, 0]
        return target - top - jnp.log(total)

    grouped = hidden.reshape(N_DP, GROUP_ROWS, D)
    grouped_ids = tokens.reshape(N_DP, GROUP_ROWS)
    logprob = lax.map(one_group, (grouped, grouped_ids)).reshape(ROWS)
    return logprob, new_weight
```

```python
import functools

import jax
import jax.numpy as jnp
from jax import lax
from jax.experimental import pallas as pl
from jax.experimental.pallas import tpu as pltpu
from jax.sharding import Mesh
from jax.sharding import PartitionSpec as P

AXES = ("x", "ylo", "z", "yhi", "c")
DP = ("x", "ylo")
VOCAB = ("z", "yhi", "c")
MESH = pl.DeviceIdType.MESH

CHUNKS = 36
HALVES = 3
BLOCK = 128
LAG_SWAP, LAG_X, LAG_FAR, LAG_Z, LAG_RELAY, LAG_Y, LAG_X2 = 1, 2, 4, 6, 8, 10, 12
STEPS = CHUNKS + LAG_X2
STEP_NEAR, STEP_FAR, STEP_OWN, STEP_OTHER = 7, 13, 18, 39
STEP_HIDDEN, EVERY, STEP_ARRIVED = 1, 2, 11
PIECES = 4
VOCAB_TILES = 3
LANES = 128
WRITES = 8

(S_HALF, S_SWAP, S_X, S_FAR, S_Z, S_RELAY, S_Y, S_X2, S_HZ, S_HFAR, S_HC, S_HY, S_HC2,
 S_TOK, S_STAT, N_SEND) = range(16)
(R_X2, R_HZ, R_HFAR, R_HC, R_HC2, R_TOK, R_STAT, R_OWN, R_OWN_TOK, R_WEIGHT, N_ONE) = range(11)


def kernel(hid, tok, old, new, out, logprob, halves, merged, near, relay, rows_all, weight, logits,
           stats, got, tokens, send, one, half_in, swap_in, x_in, far_in, relay_in, z_in, y_in, hy_in):
    x, ylo, z, yhi, c = (lax.axis_index(a) for a in AXES)
    nx, nz = lax.axis_size("x"), lax.axis_size("z")
    up_x, down_x = lax.rem(x + 1, nx), lax.rem(x + nx - 1, nx)
    up_z, down_z = lax.rem(z + 1, nz), lax.rem(z + nz - 1, nz)
    far_z = lax.rem(z + 2, nz)
    other = 1 - c
    swaps = ylo != yhi
    flip = {"yhi": 1 - yhi, "ylo": 1 - ylo}
    my_rows, cols = merged.shape
    size = my_rows // CHUNKS
    part = my_rows // HALVES
    own = hid.shape[0]
    sub = own // PIECES

    def remote(src, dst, s, recv, device):
        return pltpu.make_async_remote_copy(
            src_ref=src, dst_ref=dst, send_sem=send.at[s], recv_sem=recv,
            device_id=device, device_id_type=MESH)

    def landed(ref, sem):
        pltpu.make_async_copy(ref, ref, sem).wait()

    def at(k):
        return pl.ds(pl.multiple_of(k * size, size), size)

    def col(zs, low):
        return pl.ds(pl.multiple_of((2 * zs + low) * cols, LANES), cols)

    barrier = pltpu.get_barrier_semaphore()
    peers = [{"x": up_x}, {"x": down_x}, {"ylo": 1 - ylo}]
    for dz in range(4):
        for same in (True, False):
            for dc in range(2):
                if dz == 0 and same and dc == 0:
                    continue
                peer = {"z": lax.rem(z + dz, nz), "c": lax.rem(c + dc, 2)}
                peers.append(peer if same else {**peer, **flip})
    for peer in peers:
        pl.semaphore_signal(barrier, inc=1, device_id=peer, device_id_type=MESH)
    pl.semaphore_wait(barrier, len(peers))

    for q in range(HALVES):
        here = pl.ds(pl.multiple_of(c * my_rows + q * part, part), part)
        there = pl.ds(pl.multiple_of(other * my_rows + q * part, part), part)
        mine = halves.at[c, :, pl.ds(q * part, part)]
        remote(new.at[:, there], mine, S_HALF, half_in.at[q], {"c": other}).start()
        pltpu.make_async_copy(new.at[:, here], mine, half_in.at[q]).start()
    own_block = rows_all.at[0, z, c]
    for device in (up_z, down_z):
        remote(hid, own_block, S_HZ, one.at[R_HZ], {"z": device}).start()
    pltpu.make_async_copy(hid, own_block, one.at[R_OWN]).start()
    pltpu.make_async_copy(tok, tokens.at[0], one.at[R_OWN_TOK]).start()
    remote(tok, tokens.at[1], S_TOK, one.at[R_TOK], flip).start()
    load_weight = pltpu.make_async_copy(old, weight, one.at[R_WEIGHT])
    load_weight.start()
    landed(rows_all.at[0, z, c], one.at[R_OWN])
    landed(tokens.at[0], one.at[R_OWN_TOK])
    remote(own_block, own_block, S_HC, one.at[R_HC], {"c": other}).start()

    def merge(k):
        @pl.when(lax.rem(k, CHUNKS // HALVES) == 0)
        def _():
            q = k // (CHUNKS // HALVES)
            landed(halves.at[:, :, pl.ds(pl.multiple_of(q * part, part), part)], half_in.at[q])

        @pl.when(lax.rem(k, BLOCK // size) == 0)
        def _():
            ids = pl.ds(pl.multiple_of(k * size, BLOCK), BLOCK)
            both = jnp.concatenate([halves[0, :, ids], halves[1, :, ids]], axis=0)
            merged[ids, :] = both.T

    def swap(k):
        mine = near.at[x, at(k)]

        @pl.when(swaps)
        def _():
            remote(merged.at[at(k)], mine, S_SWAP, swap_in.at[k], flip).start()

        @pl.when(jnp.logical_not(swaps))
        def _():
            pltpu.make_async_copy(merged.at[at(k)], mine, swap_in.at[k]).start()

    def along_x(k):
        mine = near.at[x, at(k)]
        landed(mine, swap_in.at[k])
        remote(mine, mine, S_X, x_in.at[k], {"x": up_x}).start()
        remote(mine, mine, S_X, x_in.at[k], {"x": down_x}).start()

    def direction(k):
        return 1 - 2 * lax.rem(k, 2)

    def far_x(k):
        landed(near.at[pl.ds(0, 2), at(k)], x_in.at[k])
        d = direction(k)
        piece = near.at[lax.rem(x + nx - d, nx), at(k)]
        remote(piece, piece, S_FAR, far_in.at[k], {"x": lax.rem(x + nx + d, nx)}).start()

    def along_z(k):
        landed(near.at[0, at(k)], far_in.at[k])
        d = direction(k)
        target = out.at[at(k), col(z, ylo)]
        remote(near.at[far_z, at(k)], relay.at[at(k)], S_Z, relay_in.at[k],
               {"z": lax.rem(z + nz + d, nz)}).start()
        remote(near.at[up_z, at(k)], target, S_Z, z_in.at[k], {"z": up_z}).start()
        remote(near.at[down_z, at(k)], target, S_Z, z_in.at[k], {"z": down_z}).start()
        pltpu.make_async_copy(near.at[z, at(k)], target, z_in.at[k]).start()

    def relay_z(k):
        landed(relay.at[at(k)], relay_in.at[k])
        d = direction(k)
        source = lax.rem(z + nz - d, nz)
        remote(relay.at[at(k)], out.at[at(k), col(source, ylo)], S_RELAY, z_in.at[k],
               {"z": lax.rem(z + nz + d, nz)}).start()

    def along_y(k):
        landed(out.at[at(k), pl.ds(0, 4 * cols)], z_in.at[k])
        for add in (0, 2):
            piece = out.at[at(k), col(lax.rem(x, 2) + add, ylo)]
            remote(piece, piece, S_Y, y_in.at[k], {"ylo": 1 - ylo}).start()

    def along_x2(k):
        landed(out.at[at(k), pl.ds(0, 2 * cols)], y_in.at[k])
        for add, device in ((0, up_x), (2, down_x)):
            piece = out.at[at(k), col(lax.rem(x, 2) + add, 1 - ylo)]
            remote(piece, piece, S_X2, one.at[R_X2], {"x": device}).start()

    def near_hidden():
        landed(rows_all.at[0, pl.ds(0, 2), 0], one.at[R_HZ])
        for source, device, first in ((down_z, up_z, 0), (up_z, down_z, own // 2)):
            piece = rows_all.at[0, source, c, pl.ds(first, own // 2)]
            remote(piece, piece, S_HFAR, one.at[R_HFAR], {"z": device}).start()
        for source in (down_z, up_z):
            block = rows_all.at[0, source, c]
            remote(block, block, S_HC, one.at[R_HC], {"c": other}).start()

    def far_hidden():
        landed(rows_all.at[0, 0, 0], one.at[R_HFAR])
        block = rows_all.at[0, far_z, c]
        remote(block, block, S_HC, one.at[R_HC], {"c": other}).start()

    def offset_of(b):
        return lax.rem(b * (7 - b) // 2, 4)

    def hidden_y(j):
        b = j // PIECES
        source = lax.rem(z + offset_of(b), nz)
        lines = pl.ds(pl.multiple_of(lax.rem(j, PIECES) * sub, sub), sub)
        remote(rows_all.at[0, source, c, lines], rows_all.at[1, source, c, lines], S_HY,
               hy_in.at[b], flip).start()

    def hidden_y_in(b):
        block = rows_all.at[1, lax.rem(z + offset_of(b), nz), c]
        landed(block, hy_in.at[b])
        remote(block, block, S_HC2, one.at[R_HC2], {"c": other}).start()

    tile = weight.shape[0] // VOCAB_TILES
    wide = 4 * own
    first_id = ((z * 2 + yhi) * 2 + c) * weight.shape[0]

    def dot_step(nb, m):
        lines = pl.ds(pl.multiple_of(m * tile, tile), tile)
        rows = rows_all[nb // 2, pl.ds(lax.rem(nb, 2) * 2, 2)].reshape(wide, hid.shape[1])
        logits[lines, :] = lax.dot_general(
            weight[lines, :], rows, (((1,), (1,)), ((), ())),
            preferred_element_type=jnp.float32)

    def stat_step(nb):
        side = nb // 2
        high = yhi + side - 2 * yhi * side
        for i in range(2):
            zs = lax.rem(nb, 2) * 2 + i
            values = logits[:, i * LANES:(i + 1) * LANES]
            top = jnp.max(values, axis=0, keepdims=True)
            total = jnp.sum(jnp.exp(values - top), axis=0, keepdims=True)
            wanted = tokens[side, pl.ds(zs * 2 + high, 1), :] - first_id
            ids = lax.broadcasted_iota(jnp.int32, values.shape, 0)
            hit = jnp.sum(jnp.where(ids == wanted, values, 0.0), axis=0, keepdims=True)
            slot = side * 4 + zs
            stats[slot, 0:1, :] = top
            stats[slot, 1:2, :] = total
            stats[slot, 2:3, :] = hit

    def compute(first, e):
        nb, m = first + e // (VOCAB_TILES + 1), lax.rem(e, VOCAB_TILES + 1)

        @pl.when(m < VOCAB_TILES)
        def _():
            dot_step(nb, m)

        @pl.when(m == VOCAB_TILES)
        def _():
            stat_step(nb)

    events = 2 * (VOCAB_TILES + 1)

    def step(t, carry):
        stages = ((LAG_X2, along_x2), (LAG_Y, along_y), (LAG_RELAY, relay_z), (LAG_Z, along_z),
                  (LAG_FAR, far_x), (LAG_X, along_x), (LAG_SWAP, swap), (0, merge))
        for lag, stage in stages:
            k = t - lag

            @pl.when(jnp.logical_and(k >= 0, k < CHUNKS))
            def _(stage=stage, k=k):
                stage(k)

        pl.when(t == STEP_NEAR)(near_hidden)
        pl.when(t == STEP_FAR)(far_hidden)

        piece = t - STEP_HIDDEN

        @pl.when((piece >= 0) & (lax.rem(piece, EVERY) == 0) & (piece < 4 * PIECES * EVERY))
        def _():
            hidden_y(piece // EVERY)

        block = t - STEP_ARRIVED
        period = PIECES * EVERY

        @pl.when((block >= 0) & (lax.rem(block, period) == 0) & (block < 4 * period))
        def _():
            hidden_y_in(block // period)

        @pl.when(t == STEP_OWN)
        def _():
            landed(rows_all.at[0, :, 0], one.at[R_HC])
            landed(weight, one.at[R_WEIGHT])
            landed(tokens.at[1], one.at[R_TOK])

        @pl.when(t == STEP_OTHER)
        def _():
            landed(rows_all.at[1, :, 0], one.at[R_HC2])

        @pl.when((t >= STEP_OWN) & (t < STEP_OWN + events))
        def _():
            compute(0, t - STEP_OWN)

        @pl.when((t >= STEP_OTHER) & (t < STEP_OTHER + events))
        def _():
            compute(2, t - STEP_OTHER)
        return carry

    lax.fori_loop(0, STEPS, step, 0)

    for side in range(2):
        for dz in range(4):
            for dc in range(2):
                zs = lax.rem(z + dz, nz)
                src = stats.at[side * 4 + zs]
                dst = got.at[(side * 4 + z) * 2 + c]
                if side == 0 and dz == 0 and dc == 0:
                    pltpu.make_async_copy(src, dst, one.at[R_STAT]).start()
                else:
                    peer = {"z": zs, "c": lax.rem(c + dc, 2)}
                    remote(src, dst, S_STAT, one.at[R_STAT], peer if side == 0 else {**peer, **flip}).start()
    landed(got, one.at[R_STAT])
    tops = got[:, 0, :]
    top = jnp.max(tops, axis=0, keepdims=True)
    total = jnp.sum(got[:, 1, :] * jnp.exp(tops - top), axis=0, keepdims=True)
    target = jnp.sum(got[:, 2, :], axis=0, keepdims=True)
    logprob[...] = target - top - jnp.log(total)

    landed(out.at[:, pl.ds(0, 2 * cols)], one.at[R_X2])
    landed(halves.at[0], send.at[S_HALF])
    pl.when(swaps)(lambda: landed(merged, send.at[S_SWAP]))
    landed(near.at[pl.ds(0, 2)], send.at[S_X])
    landed(near.at[0], send.at[S_FAR])
    landed(near.at[pl.ds(0, 3)], send.at[S_Z])
    landed(relay, send.at[S_RELAY])
    landed(near.at[pl.ds(0, 2)], send.at[S_Y])
    landed(near.at[pl.ds(0, 2)], send.at[S_X2])
    landed(rows_all.at[0, pl.ds(0, 2), 0], send.at[S_HZ])
    landed(rows_all.at[0, 0, 0], send.at[S_HFAR])
    landed(rows_all.at[0, :, 0], send.at[S_HC])
    landed(rows_all.at[0, :, 0], send.at[S_HY])
    landed(rows_all.at[0, :, 0], send.at[S_HC2])
    landed(tokens.at[0], send.at[S_TOK])
    landed(got.at[pl.ds(0, 15)], send.at[S_STAT])


def write_out(held, both, out, both_out, sem):
    part = held.shape[0] // WRITES
    copies = [pltpu.make_async_copy(held.at[pl.ds(i * part, part)], out.at[pl.ds(i * part, part)], sem.at[i])
              for i in range(WRITES)]
    for copy in copies:
        copy.start()
    both_out[...] = both[...]
    for copy in copies:
        copy.wait()


def on_device(hidden, tokens, old_weight, new_weight):
    own, width = hidden.shape
    vocab_rows = old_weight.shape[0]
    cols = 2 * new_weight.shape[1]
    sems = pltpu.SemaphoreType.DMA
    engine_weight, both = pl.pallas_call(
        kernel,
        out_shape=(
            pltpu.VMEM((vocab_rows, width), jnp.bfloat16),
            jax.ShapeDtypeStruct((1, LANES), jnp.float32),
        ),
        in_specs=[pl.BlockSpec(memory_space=pl.ANY)] * 4,
        out_specs=(pl.BlockSpec(memory_space=pltpu.VMEM), pl.BlockSpec(memory_space=pltpu.VMEM)),
        scratch_shapes=[
            pltpu.VMEM((2, cols // 2, vocab_rows), jnp.bfloat16),
            pltpu.VMEM((vocab_rows, cols), jnp.bfloat16),
            pltpu.VMEM((4, vocab_rows, cols), jnp.bfloat16),
            pltpu.VMEM((vocab_rows, cols), jnp.bfloat16),
            pltpu.VMEM((2, 4, 2, own, width), jnp.bfloat16),
            pltpu.VMEM((vocab_rows, width), jnp.bfloat16),
            pltpu.VMEM((vocab_rows, 4 * own), jnp.float32),
            pltpu.VMEM((8, 8, LANES), jnp.float32),
            pltpu.VMEM((16, 8, LANES), jnp.float32),
            pltpu.VMEM((2, 8, LANES), jnp.int32),
            sems((N_SEND,)),
            sems((N_ONE,)),
            sems((HALVES,)),
            sems((CHUNKS,)),
            sems((CHUNKS,)),
            sems((CHUNKS,)),
            sems((CHUNKS,)),
            sems((CHUNKS,)),
            sems((CHUNKS,)),
            sems((4,)),
        ],
        compiler_params=pltpu.CompilerParams(
            collective_id=0, has_side_effects=True, vmem_limit_bytes=40 * 2**20
        ),
    )(hidden, tokens.reshape(8, LANES), old_weight, new_weight.T)
    engine_weight, both = pl.pallas_call(
        write_out,
        out_shape=(
            jax.ShapeDtypeStruct((vocab_rows, width), jnp.bfloat16),
            jax.ShapeDtypeStruct((1, LANES), jnp.float32),
        ),
        in_specs=[pl.BlockSpec(memory_space=pl.ANY), pl.BlockSpec(memory_space=pltpu.VMEM)],
        out_specs=(pl.BlockSpec(memory_space=pl.ANY), pl.BlockSpec(memory_space=pltpu.VMEM)),
        scratch_shapes=[sems((WRITES,))],
        compiler_params=pltpu.CompilerParams(vmem_limit_bytes=2**20),
    )(engine_weight, both)
    logprob = lax.dynamic_slice(both, (0, lax.axis_index("c") * own), (1, own))
    return logprob.reshape(own), engine_weight


def solution(mesh):
    finer = Mesh(mesh.devices.reshape(4, 2, 4, 2, 2), AXES)
    return jax.shard_map(
        on_device,
        mesh=finer,
        in_specs=(P(DP + VOCAB, None), P(DP), P(VOCAB, None), P(DP, VOCAB)),
        out_specs=(P(DP + VOCAB), P(VOCAB, None)),
        check_vma=False,
    )
```

```python
import functools

import jax
import jax.numpy as jnp
from jax import lax
from jax.experimental import pallas as pl
from jax.experimental.pallas import tpu as pltpu
from jax.sharding import Mesh
from jax.sharding import PartitionSpec as P

AXES = ("x", "ylo", "z", "yhi", "c")
DP = ("x", "ylo")
VOCAB = ("z", "yhi", "c")
MESH = pl.DeviceIdType.MESH

CHUNKS = 18
HALVES = 3
BLOCK = 128
LAG_SWAP, LAG_X, LAG_FAR, LAG_Z, LAG_RELAY, LAG_Y, LAG_X2 = 1, 8, 12, 17, 19, 21, 27
STEP_NEAR, STEP_FAR, STEP_OWN, STEP_OTHER = 12, 21, 22, 31
STEP_HIDDEN, EVERY, STEP_ARRIVED = 21, 1, 29
PIECES = 4
PERIOD = PIECES * EVERY
VOCAB_TILES = 3
STEPS = max(CHUNKS + LAG_X2, STEP_OTHER + 3 * PERIOD + VOCAB_TILES + 1)
LANES = 128
WRITES = 8

(S_HALF, S_SWAP, S_X, S_FAR, S_Z, S_RELAY, S_Y, S_X2, S_HZ, S_HFAR, S_HC, S_HY, S_HC2,
 S_TOK, S_STAT, N_SEND) = range(16)
(R_X2, R_HZ, R_HFAR, R_HC,  R_TOK, R_STAT, R_OWN, R_OWN_TOK, R_WEIGHT, N_ONE) = range(10)


def kernel(hid, tok, old, new, out, logprob, halves, merged, near, relay, rows_all, weight, logits,
           stats, got, tokens, send, one, half_in, swap_in, x_in, far_in, relay_in, z_in, y_in, hy_in, hc2_in):
    x, ylo, z, yhi, c = (lax.axis_index(a) for a in AXES)
    nx, nz = lax.axis_size("x"), lax.axis_size("z")
    up_x, down_x = lax.rem(x + 1, nx), lax.rem(x + nx - 1, nx)
    up_z, down_z = lax.rem(z + 1, nz), lax.rem(z + nz - 1, nz)
    far_z = lax.rem(z + 2, nz)
    other = 1 - c
    swaps = ylo != yhi
    flip = {"yhi": 1 - yhi, "ylo": 1 - ylo}
    my_rows, cols = merged.shape
    size = my_rows // CHUNKS
    part = my_rows // HALVES
    own = hid.shape[0]
    sub = own // PIECES

    def remote(src, dst, s, recv, device):
        return pltpu.make_async_remote_copy(
            src_ref=src, dst_ref=dst, send_sem=send.at[s], recv_sem=recv,
            device_id=device, device_id_type=MESH)

    def landed(ref, sem):
        pltpu.make_async_copy(ref, ref, sem).wait()

    def at(k):
        return pl.ds(pl.multiple_of(k * size, size), size)

    def col(zs, low):
        return pl.ds(pl.multiple_of((2 * zs + low) * cols, LANES), cols)

    barrier = pltpu.get_barrier_semaphore()
    peers = [{"x": up_x}, {"x": down_x}, {"ylo": 1 - ylo}]
    for dz in range(4):
        for same in (True, False):
            for dc in range(2):
                if dz == 0 and same and dc == 0:
                    continue
                peer = {"z": lax.rem(z + dz, nz), "c": lax.rem(c + dc, 2)}
                peers.append(peer if same else {**peer, **flip})
    for peer in peers:
        pl.semaphore_signal(barrier, inc=1, device_id=peer, device_id_type=MESH)
    pl.semaphore_wait(barrier, len(peers))

    for q in range(HALVES):
        here = pl.ds(pl.multiple_of(c * my_rows + q * part, part), part)
        there = pl.ds(pl.multiple_of(other * my_rows + q * part, part), part)
        mine = halves.at[c, :, pl.ds(q * part, part)]
        remote(new.at[:, there], mine, S_HALF, half_in.at[q], {"c": other}).start()
        pltpu.make_async_copy(new.at[:, here], mine, half_in.at[q]).start()
    own_block = rows_all.at[0, z, c]
    for device in (up_z, down_z):
        remote(hid, own_block, S_HZ, one.at[R_HZ], {"z": device}).start()
    pltpu.make_async_copy(hid, own_block, one.at[R_OWN]).start()
    pltpu.make_async_copy(tok, tokens.at[0], one.at[R_OWN_TOK]).start()
    remote(tok, tokens.at[1], S_TOK, one.at[R_TOK], flip).start()
    load_weight = pltpu.make_async_copy(old, weight, one.at[R_WEIGHT])
    load_weight.start()
    landed(rows_all.at[0, z, c], one.at[R_OWN])
    landed(tokens.at[0], one.at[R_OWN_TOK])
    remote(own_block, own_block, S_HC, one.at[R_HC], {"c": other}).start()

    def merge(k):
        @pl.when(lax.rem(k, CHUNKS // HALVES) == 0)
        def _():
            q = k // (CHUNKS // HALVES)
            landed(halves.at[:, :, pl.ds(pl.multiple_of(q * part, part), part)], half_in.at[q])

        @pl.when(lax.rem(k, BLOCK // size) == 0)
        def _():
            ids = pl.ds(pl.multiple_of(k * size, BLOCK), BLOCK)
            both = jnp.concatenate([halves[0, :, ids], halves[1, :, ids]], axis=0)
            merged[ids, :] = both.T

    def swap(k):
        mine = near.at[x, at(k)]

        @pl.when(swaps)
        def _():
            remote(merged.at[at(k)], mine, S_SWAP, swap_in.at[k], flip).start()

        @pl.when(jnp.logical_not(swaps))
        def _():
            pltpu.make_async_copy(merged.at[at(k)], mine, swap_in.at[k]).start()

    def along_x(k):
        mine = near.at[x, at(k)]
        landed(mine, swap_in.at[k])
        remote(mine, mine, S_X, x_in.at[k], {"x": up_x}).start()
        remote(mine, mine, S_X, x_in.at[k], {"x": down_x}).start()

    def direction(k):
        return 1 - 2 * lax.rem(k, 2)

    def far_x(k):
        landed(near.at[pl.ds(0, 2), at(k)], x_in.at[k])
        d = direction(k)
        piece = near.at[lax.rem(x + nx - d, nx), at(k)]
        remote(piece, piece, S_FAR, far_in.at[k], {"x": lax.rem(x + nx + d, nx)}).start()

    def along_z(k):
        landed(near.at[0, at(k)], far_in.at[k])
        d = direction(k)
        target = out.at[at(k), col(z, ylo)]
        remote(near.at[far_z, at(k)], relay.at[at(k)], S_Z, relay_in.at[k],
               {"z": lax.rem(z + nz + d, nz)}).start()
        remote(near.at[up_z, at(k)], target, S_Z, z_in.at[k], {"z": up_z}).start()
        remote(near.at[down_z, at(k)], target, S_Z, z_in.at[k], {"z": down_z}).start()
        pltpu.make_async_copy(near.at[z, at(k)], target, z_in.at[k]).start()

    def relay_z(k):
        landed(relay.at[at(k)], relay_in.at[k])
        d = direction(k)
        source = lax.rem(z + nz - d, nz)
        remote(relay.at[at(k)], out.at[at(k), col(source, ylo)], S_RELAY, z_in.at[k],
               {"z": lax.rem(z + nz + d, nz)}).start()

    def along_y(k):
        landed(out.at[at(k), pl.ds(0, 4 * cols)], z_in.at[k])
        for add in (0, 2):
            piece = out.at[at(k), col(lax.rem(x, 2) + add, ylo)]
            remote(piece, piece, S_Y, y_in.at[k], {"ylo": 1 - ylo}).start()

    def along_x2(k):
        landed(out.at[at(k), pl.ds(0, 2 * cols)], y_in.at[k])
        for add, device in ((0, up_x), (2, down_x)):
            piece = out.at[at(k), col(lax.rem(x, 2) + add, 1 - ylo)]
            remote(piece, piece, S_X2, one.at[R_X2], {"x": device}).start()

    def near_hidden():
        landed(rows_all.at[0, pl.ds(0, 2), 0], one.at[R_HZ])
        for source, device, first in ((down_z, up_z, 0), (up_z, down_z, own // 2)):
            piece = rows_all.at[0, source, c, pl.ds(first, own // 2)]
            remote(piece, piece, S_HFAR, one.at[R_HFAR], {"z": device}).start()
        for source in (down_z, up_z):
            block = rows_all.at[0, source, c]
            remote(block, block, S_HC, one.at[R_HC], {"c": other}).start()

    def far_hidden():
        landed(rows_all.at[0, 0, 0], one.at[R_HFAR])
        block = rows_all.at[0, far_z, c]
        remote(block, block, S_HC, one.at[R_HC], {"c": other}).start()

    def offset_of(b):
        return lax.rem(b * (7 - b) // 2, 4)

    def hidden_y(j):
        b = j // PIECES
        source = lax.rem(z + offset_of(b), nz)
        lines = pl.ds(pl.multiple_of(lax.rem(j, PIECES) * sub, sub), sub)
        remote(rows_all.at[0, source, c, lines], rows_all.at[1, source, c, lines], S_HY,
               hy_in.at[b], flip).start()

    def hidden_y_in(b):
        block = rows_all.at[1, lax.rem(z + offset_of(b), nz), c]
        landed(block, hy_in.at[b])
        remote(block, block, S_HC2, hc2_in.at[b], {"c": other}).start()

    tile = weight.shape[0] // VOCAB_TILES
    first_id = ((z * 2 + yhi) * 2 + c) * weight.shape[0]

    def dot_step(m, rows, lanes):
        lines = pl.ds(pl.multiple_of(m * tile, tile), tile)
        logits[lines, 0:lanes] = lax.dot_general(
            weight[lines, :], rows.reshape(lanes, hid.shape[1]), (((1,), (1,)), ((), ())),
            preferred_element_type=jnp.float32)

    def stat_step(side, zs, first):
        high = 1 - yhi if side else yhi
        values = logits[:, first:first + LANES]
        top = jnp.max(values, axis=0, keepdims=True)
        total = jnp.sum(jnp.exp(values - top), axis=0, keepdims=True)
        wanted = tokens[side, pl.ds(zs * 2 + high, 1), :] - first_id
        ids = lax.broadcasted_iota(jnp.int32, values.shape, 0)
        hit = jnp.sum(jnp.where(ids == wanted, values, 0.0), axis=0, keepdims=True)
        slot = side * 4 + zs
        stats[slot, 0:1, :] = top
        stats[slot, 1:2, :] = total
        stats[slot, 2:3, :] = hit

    def compute_own(e):
        pair, m = e // (VOCAB_TILES + 1), lax.rem(e, VOCAB_TILES + 1)

        @pl.when(m < VOCAB_TILES)
        def _():
            dot_step(m, rows_all[0, pl.ds(pair * 2, 2)], 2 * LANES)

        @pl.when(m == VOCAB_TILES)
        def _():
            for i in range(2):
                stat_step(0, pair * 2 + i, i * LANES)

    def compute_other(e):
        b, m = e // PERIOD, lax.rem(e, PERIOD)
        zs = lax.rem(z + offset_of(b), nz)

        @pl.when(m == 0)
        def _():
            landed(rows_all.at[1, 0, 0], hc2_in.at[b])

        @pl.when(m < VOCAB_TILES)
        def _():
            dot_step(m, rows_all[1, zs], LANES)

        @pl.when(m == VOCAB_TILES)
        def _():
            stat_step(1, zs, 0)

    events = 2 * (VOCAB_TILES + 1)

    def step(t, carry):
        stages = ((LAG_X2, along_x2), (LAG_Y, along_y), (LAG_RELAY, relay_z), (LAG_Z, along_z),
                  (LAG_FAR, far_x), (LAG_X, along_x), (LAG_SWAP, swap), (0, merge))
        for lag, stage in stages:
            k = t - lag

            @pl.when(jnp.logical_and(k >= 0, k < CHUNKS))
            def _(stage=stage, k=k):
                stage(k)

        pl.when(t == STEP_NEAR)(near_hidden)
        pl.when(t == STEP_FAR)(far_hidden)

        piece = t - STEP_HIDDEN

        @pl.when((piece >= 0) & (lax.rem(piece, EVERY) == 0) & (piece < 4 * PIECES * EVERY))
        def _():
            hidden_y(piece // EVERY)

        block = t - STEP_ARRIVED

        @pl.when((block >= 0) & (lax.rem(block, PERIOD) == 0) & (block < 4 * PERIOD))
        def _():
            hidden_y_in(block // PERIOD)

        @pl.when(t == STEP_OWN)
        def _():
            landed(rows_all.at[0, :, 0], one.at[R_HC])
            landed(weight, one.at[R_WEIGHT])
            landed(tokens.at[1], one.at[R_TOK])

        @pl.when((t >= STEP_OWN) & (t < STEP_OWN + events))
        def _():
            compute_own(t - STEP_OWN)

        @pl.when((t >= STEP_OTHER) & (t < STEP_OTHER + 4 * PERIOD))
        def _():
            compute_other(t - STEP_OTHER)
        return carry

    lax.fori_loop(0, STEPS, step, 0)

    for side in range(2):
        for dz in range(4):
            for dc in range(2):
                zs = lax.rem(z + dz, nz)
                src = stats.at[side * 4 + zs]
                dst = got.at[(side * 4 + z) * 2 + c]
                if side == 0 and dz == 0 and dc == 0:
                    pltpu.make_async_copy(src, dst, one.at[R_STAT]).start()
                else:
                    peer = {"z": zs, "c": lax.rem(c + dc, 2)}
                    remote(src, dst, S_STAT, one.at[R_STAT], peer if side == 0 else {**peer, **flip}).start()
    landed(got, one.at[R_STAT])
    tops = got[:, 0, :]
    top = jnp.max(tops, axis=0, keepdims=True)
    total = jnp.sum(got[:, 1, :] * jnp.exp(tops - top), axis=0, keepdims=True)
    target = jnp.sum(got[:, 2, :], axis=0, keepdims=True)
    logprob[...] = target - top - jnp.log(total)

    landed(out.at[:, pl.ds(0, 2 * cols)], one.at[R_X2])
    landed(halves.at[0], send.at[S_HALF])
    pl.when(swaps)(lambda: landed(merged, send.at[S_SWAP]))
    landed(near.at[pl.ds(0, 2)], send.at[S_X])
    landed(near.at[0], send.at[S_FAR])
    landed(near.at[pl.ds(0, 3)], send.at[S_Z])
    landed(relay, send.at[S_RELAY])
    landed(near.at[pl.ds(0, 2)], send.at[S_Y])
    landed(near.at[pl.ds(0, 2)], send.at[S_X2])
    landed(rows_all.at[0, pl.ds(0, 2), 0], send.at[S_HZ])
    landed(rows_all.at[0, 0, 0], send.at[S_HFAR])
    landed(rows_all.at[0, :, 0], send.at[S_HC])
    landed(rows_all.at[0, :, 0], send.at[S_HY])
    landed(rows_all.at[0, :, 0], send.at[S_HC2])
    landed(tokens.at[0], send.at[S_TOK])
    landed(got.at[pl.ds(0, 15)], send.at[S_STAT])


def write_out(held, both, out, both_out, sem):
    part = held.shape[0] // WRITES
    copies = [pltpu.make_async_copy(held.at[pl.ds(i * part, part)], out.at[pl.ds(i * part, part)], sem.at[i])
              for i in range(WRITES)]
    for copy in copies:
        copy.start()
    both_out[...] = both[...]
    for copy in copies:
        copy.wait()


def on_device(hidden, tokens, old_weight, new_weight):
    own, width = hidden.shape
    vocab_rows = old_weight.shape[0]
    cols = 2 * new_weight.shape[1]
    sems = pltpu.SemaphoreType.DMA
    engine_weight, both = pl.pallas_call(
        kernel,
        out_shape=(
            pltpu.VMEM((vocab_rows, width), jnp.bfloat16),
            jax.ShapeDtypeStruct((1, LANES), jnp.float32),
        ),
        in_specs=[pl.BlockSpec(memory_space=pltpu.HBM)] * 4,
        out_specs=(pl.BlockSpec(memory_space=pltpu.VMEM), pl.BlockSpec(memory_space=pltpu.VMEM)),
        scratch_shapes=[
            pltpu.VMEM((2, cols // 2, vocab_rows), jnp.bfloat16),
            pltpu.VMEM((vocab_rows, cols), jnp.bfloat16),
            pltpu.VMEM((4, vocab_rows, cols), jnp.bfloat16),
            pltpu.VMEM((vocab_rows, cols), jnp.bfloat16),
            pltpu.VMEM((2, 4, 2, own, width), jnp.bfloat16),
            pltpu.VMEM((vocab_rows, width), jnp.bfloat16),
            pltpu.VMEM((vocab_rows, 4 * own), jnp.float32),
            pltpu.VMEM((8, 8, LANES), jnp.float32),
            pltpu.VMEM((16, 8, LANES), jnp.float32),
            pltpu.VMEM((2, 8, LANES), jnp.int32),
            sems((N_SEND,)),
            sems((N_ONE,)),
            sems((HALVES,)),
            sems((CHUNKS,)),
            sems((CHUNKS,)),
            sems((CHUNKS,)),
            sems((CHUNKS,)),
            sems((CHUNKS,)),
            sems((CHUNKS,)),
            sems((4,)),
            sems((4,)),
        ],
        compiler_params=pltpu.CompilerParams(
            collective_id=0, has_side_effects=True, vmem_limit_bytes=40 * 2**20
        ),
    )(*(pltpu.with_memory_space_constraint(a, pltpu.HBM) for a in (hidden, tokens.reshape(8, LANES), old_weight, new_weight.T)))
    engine_weight, both = pl.pallas_call(
        write_out,
        out_shape=(
            jax.ShapeDtypeStruct((vocab_rows, width), jnp.bfloat16),
            jax.ShapeDtypeStruct((1, LANES), jnp.float32),
        ),
        in_specs=[pl.BlockSpec(memory_space=pl.ANY), pl.BlockSpec(memory_space=pltpu.VMEM)],
        out_specs=(pl.BlockSpec(memory_space=pl.ANY), pl.BlockSpec(memory_space=pltpu.VMEM)),
        scratch_shapes=[sems((WRITES,))],
        compiler_params=pltpu.CompilerParams(vmem_limit_bytes=2**20),
    )(engine_weight, both)
    logprob = lax.dynamic_slice(both, (0, lax.axis_index("c") * own), (1, own))
    return logprob.reshape(own), engine_weight


def solution(mesh):
    finer = Mesh(mesh.devices.reshape(4, 2, 4, 2, 2), AXES)
    return jax.shard_map(
        on_device,
        mesh=finer,
        in_specs=(P(DP + VOCAB, None), P(DP), P(VOCAB, None), P(DP, VOCAB)),
        out_specs=(P(DP + VOCAB), P(VOCAB, None)),
        check_vma=False,
    )
```

```python
import functools

import jax
import jax.numpy as jnp
from jax import lax
from jax.experimental import pallas as pl
from jax.experimental.pallas import tpu as pltpu
from jax.sharding import Mesh
from jax.sharding import PartitionSpec as P

AXES = ("x", "ylo", "z", "yhi", "c")
DP = ("x", "ylo")
VOCAB = ("z", "yhi", "c")
MESH = pl.DeviceIdType.MESH

CHUNKS = 18
HALVES = 3
BLOCK = 128
LAG_SWAP, LAG_X, LAG_FAR, LAG_Z, LAG_RELAY, LAG_Y, LAG_X2 = 2, 10, 13, 15, 17, 19, 24
ORDER = ("merge", "far_x", "x2", "y", "swap", "x", "relay", "z")
STEP_NEAR, STEP_ON, STEP_ON2, STEP_FAR, STEP_OWN, STEP_OTHER = 11, 11, 12, 16, 17, 25
STEP_HIDDEN, EVERY, STEP_ARRIVED = 12, 1, 24
EARLY = 2
PIECES = 4
PERIOD = PIECES * EVERY
VOCAB_TILES = 3
STEPS = max(CHUNKS + LAG_X2, STEP_OTHER + 3 * PERIOD + VOCAB_TILES + 1)
LANES = 128
WRITES = 8

(S_HALF, S_SWAP, S_X, S_FAR, S_Z, S_RELAY, S_Y, S_X2, S_HZ, S_HFAR, S_HC, S_HY, S_HC2,
 S_TOK, S_STAT, N_SEND) = range(16)
(R_X2, R_HZ, R_HFAR, R_HC,  R_TOK, R_STAT, R_OWN, R_OWN_TOK, R_WEIGHT, N_ONE) = range(10)


def kernel(hid, tok, old, new, out, logprob, halves, merged, near, relay, rows_all, weight, logits,
           stats, got, tokens, send, one, half_in, swap_in, x_in, far_in, relay_in, z_in, y_in, hy_in, hc2_in):
    x, ylo, z, yhi, c = (lax.axis_index(a) for a in AXES)
    nx, nz = lax.axis_size("x"), lax.axis_size("z")
    up_x, down_x = lax.rem(x + 1, nx), lax.rem(x + nx - 1, nx)
    up_z, down_z = lax.rem(z + 1, nz), lax.rem(z + nz - 1, nz)
    far_z = lax.rem(z + 2, nz)
    other = 1 - c
    swaps = ylo != yhi
    flip = {"yhi": 1 - yhi, "ylo": 1 - ylo}
    my_rows, cols = merged.shape
    size = my_rows // CHUNKS
    part = my_rows // HALVES
    own = hid.shape[0]
    sub = own // PIECES

    def remote(src, dst, s, recv, device):
        return pltpu.make_async_remote_copy(
            src_ref=src, dst_ref=dst, send_sem=send.at[s], recv_sem=recv,
            device_id=device, device_id_type=MESH)

    def landed(ref, sem):
        pltpu.make_async_copy(ref, ref, sem).wait()

    def at(k):
        return pl.ds(pl.multiple_of(k * size, size), size)

    def col(zs, low):
        return pl.ds(pl.multiple_of((2 * zs + low) * cols, LANES), cols)

    barrier = pltpu.get_barrier_semaphore()
    peers = [{"x": up_x}, {"x": down_x}, {"ylo": 1 - ylo}]
    peers += [{"z": up_z}, {"z": down_z}, {"c": other}, flip]
    for peer in peers:
        pl.semaphore_signal(barrier, inc=1, device_id=peer, device_id_type=MESH)
    pl.semaphore_wait(barrier, len(peers))

    for q in range(HALVES):
        here = pl.ds(pl.multiple_of(c * my_rows + q * part, part), part)
        there = pl.ds(pl.multiple_of(other * my_rows + q * part, part), part)
        mine = halves.at[c, :, pl.ds(q * part, part)]
        remote(new.at[:, there], mine, S_HALF, half_in.at[q], {"c": other}).start()
        pltpu.make_async_copy(new.at[:, here], mine, half_in.at[q]).start()
    own_block = rows_all.at[0, z, c]
    for j in range(EARLY):
        lines = pl.ds(j * sub, sub)
        remote(hid.at[lines], rows_all.at[1, z, c, lines], S_HY, hy_in.at[0], flip).start()
    for device in (up_z, down_z):
        remote(hid, own_block, S_HZ, one.at[R_HZ], {"z": device}).start()
    pltpu.make_async_copy(hid, own_block, one.at[R_OWN]).start()
    pltpu.make_async_copy(tok, tokens.at[0], one.at[R_OWN_TOK]).start()
    remote(tok, tokens.at[1], S_TOK, one.at[R_TOK], flip).start()
    load_weight = pltpu.make_async_copy(old, weight, one.at[R_WEIGHT])
    load_weight.start()
    landed(rows_all.at[0, z, c], one.at[R_OWN])
    landed(tokens.at[0], one.at[R_OWN_TOK])
    remote(own_block, own_block, S_HC, one.at[R_HC], {"c": other}).start()

    def merge(k):
        @pl.when(lax.rem(k, CHUNKS // HALVES) == 0)
        def _():
            q = k // (CHUNKS // HALVES)
            landed(halves.at[:, :, pl.ds(pl.multiple_of(q * part, part), part)], half_in.at[q])

        @pl.when(lax.rem(k, BLOCK // size) == 0)
        def _():
            ids = pl.ds(pl.multiple_of(k * size, BLOCK), BLOCK)
            both = jnp.concatenate([halves[0, :, ids], halves[1, :, ids]], axis=0)
            merged[ids, :] = both.T

    def swap(k):
        mine = near.at[x, at(k)]

        @pl.when(swaps)
        def _():
            remote(merged.at[at(k)], mine, S_SWAP, swap_in.at[k], flip).start()

        @pl.when(jnp.logical_not(swaps))
        def _():
            pltpu.make_async_copy(merged.at[at(k)], mine, swap_in.at[k]).start()

    def along_x(k):
        mine = near.at[x, at(k)]
        landed(mine, swap_in.at[k])
        remote(mine, mine, S_X, x_in.at[k], {"x": up_x}).start()
        remote(mine, mine, S_X, x_in.at[k], {"x": down_x}).start()

    def direction(k):
        return 1 - 2 * lax.rem(k, 2)

    def far_x(k):
        landed(near.at[pl.ds(0, 2), at(k)], x_in.at[k])
        d = direction(k)
        piece = near.at[lax.rem(x + nx - d, nx), at(k)]
        remote(piece, piece, S_FAR, far_in.at[k], {"x": lax.rem(x + nx + d, nx)}).start()

    def along_z(k):
        landed(near.at[0, at(k)], far_in.at[k])
        d = direction(k)
        target = out.at[at(k), col(z, ylo)]
        remote(near.at[far_z, at(k)], relay.at[at(k)], S_Z, relay_in.at[k],
               {"z": lax.rem(z + nz + d, nz)}).start()
        remote(near.at[up_z, at(k)], target, S_Z, z_in.at[k], {"z": up_z}).start()
        remote(near.at[down_z, at(k)], target, S_Z, z_in.at[k], {"z": down_z}).start()
        pltpu.make_async_copy(near.at[z, at(k)], target, z_in.at[k]).start()

    def relay_z(k):
        landed(relay.at[at(k)], relay_in.at[k])
        d = direction(k)
        source = lax.rem(z + nz - d, nz)
        remote(relay.at[at(k)], out.at[at(k), col(source, ylo)], S_RELAY, z_in.at[k],
               {"z": lax.rem(z + nz + d, nz)}).start()

    def along_y(k):
        landed(out.at[at(k), pl.ds(0, 4 * cols)], z_in.at[k])
        for add in (0, 2):
            piece = out.at[at(k), col(lax.rem(x, 2) + add, ylo)]
            remote(piece, piece, S_Y, y_in.at[k], {"ylo": 1 - ylo}).start()

    def along_x2(k):
        landed(out.at[at(k), pl.ds(0, 2 * cols)], y_in.at[k])
        for add, device in ((0, up_x), (2, down_x)):
            piece = out.at[at(k), col(lax.rem(x, 2) + add, 1 - ylo)]
            remote(piece, piece, S_X2, one.at[R_X2], {"x": device}).start()

    def near_hidden():
        landed(rows_all.at[0, pl.ds(0, 2), 0], one.at[R_HZ])
        for source in (down_z, up_z):
            block = rows_all.at[0, source, c]
            remote(block, block, S_HC, one.at[R_HC], {"c": other}).start()

    def hidden_on(part):
        quarter = own // 4
        for source, device, first in ((down_z, up_z, 0), (up_z, down_z, 2)):
            piece = rows_all.at[0, source, c, pl.ds((first + part) * quarter, quarter)]
            remote(piece, piece, S_HFAR, one.at[R_HFAR], {"z": device}).start()

    def far_hidden():
        landed(rows_all.at[0, 0, 0], one.at[R_HFAR])
        block = rows_all.at[0, far_z, c]
        remote(block, block, S_HC, one.at[R_HC], {"c": other}).start()

    def offset_of(b):
        return lax.rem(b * (7 - b) // 2, 4)

    def hidden_y(j):
        b = j // PIECES
        source = lax.rem(z + offset_of(b), nz)
        lines = pl.ds(pl.multiple_of(lax.rem(j, PIECES) * sub, sub), sub)
        remote(rows_all.at[0, source, c, lines], rows_all.at[1, source, c, lines], S_HY,
               hy_in.at[b], flip).start()

    def hidden_y_in(b):
        block = rows_all.at[1, lax.rem(z + offset_of(b), nz), c]
        landed(block, hy_in.at[b])
        remote(block, block, S_HC2, hc2_in.at[b], {"c": other}).start()

    tile = weight.shape[0] // VOCAB_TILES
    first_id = ((z * 2 + yhi) * 2 + c) * weight.shape[0]

    def dot_step(m, rows, lanes):
        lines = pl.ds(pl.multiple_of(m * tile, tile), tile)
        logits[lines, 0:lanes] = lax.dot_general(
            weight[lines, :], rows.reshape(lanes, hid.shape[1]), (((1,), (1,)), ((), ())),
            preferred_element_type=jnp.float32)

    def stat_step(side, zs, first):
        high = 1 - yhi if side else yhi
        values = logits[:, first:first + LANES]
        top = jnp.max(values, axis=0, keepdims=True)
        total = jnp.sum(jnp.exp(values - top), axis=0, keepdims=True)
        wanted = tokens[side, pl.ds(zs * 2 + high, 1), :] - first_id
        ids = lax.broadcasted_iota(jnp.int32, values.shape, 0)
        hit = jnp.sum(jnp.where(ids == wanted, values, 0.0), axis=0, keepdims=True)
        slot = side * 4 + zs
        stats[slot, 0:1, :] = top
        stats[slot, 1:2, :] = total
        stats[slot, 2:3, :] = hit

    def compute_own(e):
        pair, m = e // (VOCAB_TILES + 1), lax.rem(e, VOCAB_TILES + 1)

        @pl.when(m < VOCAB_TILES)
        def _():
            dot_step(m, rows_all[0, pl.ds(pair * 2, 2)], 2 * LANES)

        @pl.when(m == VOCAB_TILES)
        def _():
            for i in range(2):
                stat_step(0, pair * 2 + i, i * LANES)

    def compute_other(e):
        b, m = e // PERIOD, lax.rem(e, PERIOD)
        zs = lax.rem(z + offset_of(b), nz)

        @pl.when(m == 0)
        def _():
            landed(rows_all.at[1, 0, 0], hc2_in.at[b])

        @pl.when(m < VOCAB_TILES)
        def _():
            dot_step(m, rows_all[1, zs], LANES)

        @pl.when(m == VOCAB_TILES)
        def _():
            stat_step(1, zs, 0)

    events = 2 * (VOCAB_TILES + 1)

    def step(t, carry):
        stages = {"x2": (LAG_X2, along_x2), "y": (LAG_Y, along_y), "relay": (LAG_RELAY, relay_z),
                  "z": (LAG_Z, along_z), "far_x": (LAG_FAR, far_x), "x": (LAG_X, along_x),
                  "swap": (LAG_SWAP, swap), "merge": (0, merge)}
        for lag, stage in (stages[name] for name in ORDER):
            k = t - lag

            @pl.when(jnp.logical_and(k >= 0, k < CHUNKS))
            def _(stage=stage, k=k):
                stage(k)

        pl.when(t == STEP_NEAR)(near_hidden)
        pl.when(t == STEP_ON)(lambda: hidden_on(0))
        pl.when(t == STEP_ON2)(lambda: hidden_on(1))
        pl.when(t == STEP_FAR)(far_hidden)

        piece = t - STEP_HIDDEN

        @pl.when((piece >= EARLY * EVERY) & (lax.rem(piece, EVERY) == 0) & (piece < 4 * PIECES * EVERY))
        def _():
            hidden_y(piece // EVERY)

        block = t - STEP_ARRIVED

        @pl.when((block >= 0) & (lax.rem(block, PERIOD) == 0) & (block < 4 * PERIOD))
        def _():
            hidden_y_in(block // PERIOD)

        @pl.when(t == STEP_OWN)
        def _():
            landed(rows_all.at[0, :, 0], one.at[R_HC])
            landed(weight, one.at[R_WEIGHT])
            landed(tokens.at[1], one.at[R_TOK])

        @pl.when((t >= STEP_OWN) & (t < STEP_OWN + events))
        def _():
            compute_own(t - STEP_OWN)

        @pl.when((t >= STEP_OTHER) & (t < STEP_OTHER + 4 * PERIOD))
        def _():
            compute_other(t - STEP_OTHER)
        return carry

    lax.fori_loop(0, STEPS, step, 0)

    for side in range(2):
        for dz in range(4):
            for dc in range(2):
                zs = lax.rem(z + dz, nz)
                src = stats.at[side * 4 + zs]
                dst = got.at[(side * 4 + z) * 2 + c]
                if side == 0 and dz == 0 and dc == 0:
                    pltpu.make_async_copy(src, dst, one.at[R_STAT]).start()
                else:
                    peer = {"z": zs, "c": lax.rem(c + dc, 2)}
                    remote(src, dst, S_STAT, one.at[R_STAT], peer if side == 0 else {**peer, **flip}).start()
    landed(got, one.at[R_STAT])
    tops = got[:, 0, :]
    top = jnp.max(tops, axis=0, keepdims=True)
    total = jnp.sum(got[:, 1, :] * jnp.exp(tops - top), axis=0, keepdims=True)
    target = jnp.sum(got[:, 2, :], axis=0, keepdims=True)
    logprob[...] = target - top - jnp.log(total)

    landed(out.at[:, pl.ds(0, 2 * cols)], one.at[R_X2])
    landed(halves.at[0], send.at[S_HALF])
    pl.when(swaps)(lambda: landed(merged, send.at[S_SWAP]))
    landed(near.at[pl.ds(0, 2)], send.at[S_X])
    landed(near.at[0], send.at[S_FAR])
    landed(near.at[pl.ds(0, 3)], send.at[S_Z])
    landed(relay, send.at[S_RELAY])
    landed(near.at[pl.ds(0, 2)], send.at[S_Y])
    landed(near.at[pl.ds(0, 2)], send.at[S_X2])
    landed(rows_all.at[0, pl.ds(0, 2), 0], send.at[S_HZ])
    landed(rows_all.at[0, 0, 0], send.at[S_HFAR])
    landed(rows_all.at[0, :, 0], send.at[S_HC])
    landed(rows_all.at[0, :, 0], send.at[S_HY])
    landed(rows_all.at[0, :, 0], send.at[S_HC2])
    landed(tokens.at[0], send.at[S_TOK])
    landed(got.at[pl.ds(0, 15)], send.at[S_STAT])


def write_out(held, both, out, both_out, sem):
    part = held.shape[0] // WRITES
    copies = [pltpu.make_async_copy(held.at[pl.ds(i * part, part)], out.at[pl.ds(i * part, part)], sem.at[i])
              for i in range(WRITES)]
    for copy in copies:
        copy.start()
    values = both[...]
    mine = jnp.where(lax.axis_index("c") == 0, values, pltpu.roll(values, LANES // 2, 1))
    both_out[...] = mine[:, : LANES // 2]
    for copy in copies:
        copy.wait()


def on_device(hidden, tokens, old_weight, new_weight):
    own, width = hidden.shape
    vocab_rows = old_weight.shape[0]
    cols = 2 * new_weight.shape[1]
    sems = pltpu.SemaphoreType.DMA
    engine_weight, both = pl.pallas_call(
        kernel,
        out_shape=(
            pltpu.VMEM((vocab_rows, width), jnp.bfloat16),
            jax.ShapeDtypeStruct((1, LANES), jnp.float32),
        ),
        in_specs=[pl.BlockSpec(memory_space=pltpu.HBM)] * 4,
        out_specs=(pl.BlockSpec(memory_space=pltpu.VMEM), pl.BlockSpec(memory_space=pltpu.VMEM)),
        scratch_shapes=[
            pltpu.VMEM((2, cols // 2, vocab_rows), jnp.bfloat16),
            pltpu.VMEM((vocab_rows, cols), jnp.bfloat16),
            pltpu.VMEM((4, vocab_rows, cols), jnp.bfloat16),
            pltpu.VMEM((vocab_rows, cols), jnp.bfloat16),
            pltpu.VMEM((2, 4, 2, own, width), jnp.bfloat16),
            pltpu.VMEM((vocab_rows, width), jnp.bfloat16),
            pltpu.VMEM((vocab_rows, 4 * own), jnp.float32),
            pltpu.VMEM((8, 8, LANES), jnp.float32),
            pltpu.VMEM((16, 8, LANES), jnp.float32),
            pltpu.VMEM((2, 8, LANES), jnp.int32),
            sems((N_SEND,)),
            sems((N_ONE,)),
            sems((HALVES,)),
            sems((CHUNKS,)),
            sems((CHUNKS,)),
            sems((CHUNKS,)),
            sems((CHUNKS,)),
            sems((CHUNKS,)),
            sems((CHUNKS,)),
            sems((4,)),
            sems((4,)),
        ],
        compiler_params=pltpu.CompilerParams(
            collective_id=0, has_side_effects=True, vmem_limit_bytes=40 * 2**20
        ),
    )(*(pltpu.with_memory_space_constraint(a, pltpu.HBM) for a in (hidden, tokens.reshape(8, LANES), old_weight, new_weight.T)))
    engine_weight, logprob = pl.pallas_call(
        write_out,
        out_shape=(
            jax.ShapeDtypeStruct((vocab_rows, width), jnp.bfloat16),
            jax.ShapeDtypeStruct((1, own), jnp.float32),
        ),
        in_specs=[pl.BlockSpec(memory_space=pl.ANY), pl.BlockSpec(memory_space=pltpu.VMEM)],
        out_specs=(pl.BlockSpec(memory_space=pl.ANY), pl.BlockSpec(memory_space=pltpu.VMEM)),
        scratch_shapes=[sems((WRITES,))],
        compiler_params=pltpu.CompilerParams(vmem_limit_bytes=2**20),
    )(engine_weight, both)
    return logprob.reshape(own), engine_weight


def solution(mesh):
    finer = Mesh(mesh.devices.reshape(4, 2, 4, 2, 2), AXES)
    return jax.shard_map(
        on_device,
        mesh=finer,
        in_specs=(P(DP + VOCAB, None), P(DP), P(VOCAB, None), P(DP, VOCAB)),
        out_specs=(P(DP + VOCAB), P(VOCAB, None)),
        check_vma=False,
    )
```

```python
import functools

import jax
import jax.numpy as jnp
from jax import lax
from jax.experimental import pallas as pl
from jax.experimental.pallas import tpu as pltpu
from jax.sharding import Mesh
from jax.sharding import PartitionSpec as P

AXES = ("x", "ylo", "z", "yhi", "c")
DP = ("x", "ylo")
VOCAB = ("z", "yhi", "c")
MESH = pl.DeviceIdType.MESH

CHUNKS = 18
HALVES = 9
BLOCK = 128
LAG_SWAP, LAG_X, LAG_FAR, LAG_Z, LAG_RELAY, LAG_Y, LAG_X2 = 2, 10, 13, 15, 17, 19, 24
ORDER = ("merge", "far_x", "x2", "y", "swap", "x", "relay", "z")
STEP_NEAR, STEP_ON, STEP_ON2, STEP_FAR, STEP_OWN, STEP_OTHER = 11, 11, 12, 16, 17, 25
STEP_HIDDEN, EVERY, STEP_ARRIVED = 12, 1, 24
EARLY = 1
PIECES = 4
PERIOD = PIECES * EVERY
VOCAB_TILES = 3
STEPS = max(CHUNKS + LAG_X2, STEP_OTHER + 3 * PERIOD + VOCAB_TILES + 1)
LANES = 128
WRITES = 4

(S_HALF, S_SWAP, S_X, S_FAR, S_Z, S_RELAY, S_Y, S_X2, S_HZ, S_HFAR, S_HC, S_HY, S_HC2,
 S_TOK, S_STAT, N_SEND) = range(16)
(R_X2, R_HZ, R_HFAR, R_HC,  R_TOK, R_STAT, R_OWN, R_OWN_TOK, R_WEIGHT, N_ONE) = range(10)


def kernel(hid, tok, old, new, out, logprob, halves, merged, near, relay, rows_all, weight, logits,
           stats, got, tokens, send, one, half_in, swap_in, x_in, far_in, relay_in, z_in, y_in, hy_in, hc2_in):
    x, ylo, z, yhi, c = (lax.axis_index(a) for a in AXES)
    nx, nz = lax.axis_size("x"), lax.axis_size("z")
    up_x, down_x = lax.rem(x + 1, nx), lax.rem(x + nx - 1, nx)
    up_z, down_z = lax.rem(z + 1, nz), lax.rem(z + nz - 1, nz)
    far_z = lax.rem(z + 2, nz)
    other = 1 - c
    swaps = ylo != yhi
    flip = {"yhi": 1 - yhi, "ylo": 1 - ylo}
    my_rows, cols = merged.shape
    size = my_rows // CHUNKS
    part = my_rows // HALVES
    own = hid.shape[0]
    sub = own // PIECES

    def remote(src, dst, s, recv, device):
        return pltpu.make_async_remote_copy(
            src_ref=src, dst_ref=dst, send_sem=send.at[s], recv_sem=recv,
            device_id=device, device_id_type=MESH)

    def landed(ref, sem):
        pltpu.make_async_copy(ref, ref, sem).wait()

    def at(k):
        return pl.ds(pl.multiple_of(k * size, size), size)

    def col(zs, low):
        return pl.ds(pl.multiple_of((2 * zs + low) * cols, LANES), cols)

    barrier = pltpu.get_barrier_semaphore()
    peers = [{"x": up_x}, {"x": down_x}, {"ylo": 1 - ylo}]
    peers += [{"z": up_z}, {"z": down_z}, {"c": other}, flip]
    for peer in peers:
        pl.semaphore_signal(barrier, inc=1, device_id=peer, device_id_type=MESH)
    pl.semaphore_wait(barrier, len(peers))

    for q in range(HALVES):
        here = pl.ds(pl.multiple_of(c * my_rows + q * part, part), part)
        there = pl.ds(pl.multiple_of(other * my_rows + q * part, part), part)
        mine = halves.at[c, :, pl.ds(q * part, part)]
        remote(new.at[:, there], mine, S_HALF, half_in.at[q], {"c": other}).start()
        pltpu.make_async_copy(new.at[:, here], mine, half_in.at[q]).start()
    own_block = rows_all.at[0, z, c]
    for j in range(EARLY):
        lines = pl.ds(j * sub, sub)
        remote(hid.at[lines], rows_all.at[1, z, c, lines], S_HY, hy_in.at[0], flip).start()
    for device in (up_z, down_z):
        remote(hid, own_block, S_HZ, one.at[R_HZ], {"z": device}).start()
    pltpu.make_async_copy(hid, own_block, one.at[R_OWN]).start()
    pltpu.make_async_copy(tok, tokens.at[0], one.at[R_OWN_TOK]).start()
    remote(tok, tokens.at[1], S_TOK, one.at[R_TOK], flip).start()
    load_weight = pltpu.make_async_copy(old, weight, one.at[R_WEIGHT])
    load_weight.start()
    landed(rows_all.at[0, z, c], one.at[R_OWN])
    landed(tokens.at[0], one.at[R_OWN_TOK])
    remote(own_block, own_block, S_HC, one.at[R_HC], {"c": other}).start()

    def merge(k):
        @pl.when(lax.rem(k, CHUNKS // HALVES) == 0)
        def _():
            q = k // (CHUNKS // HALVES)
            landed(halves.at[:, :, pl.ds(pl.multiple_of(q * part, part), part)], half_in.at[q])

        @pl.when(lax.rem(k, BLOCK // size) == 0)
        def _():
            ids = pl.ds(pl.multiple_of(k * size, BLOCK), BLOCK)
            both = jnp.concatenate([halves[0, :, ids], halves[1, :, ids]], axis=0)
            merged[ids, :] = both.T

    def swap(k):
        mine = near.at[x, at(k)]

        @pl.when(swaps)
        def _():
            remote(merged.at[at(k)], mine, S_SWAP, swap_in.at[k], flip).start()

        @pl.when(jnp.logical_not(swaps))
        def _():
            pltpu.make_async_copy(merged.at[at(k)], mine, swap_in.at[k]).start()

    def along_x(k):
        mine = near.at[x, at(k)]
        landed(mine, swap_in.at[k])
        remote(mine, mine, S_X, x_in.at[k], {"x": up_x}).start()
        remote(mine, mine, S_X, x_in.at[k], {"x": down_x}).start()

    def direction(k):
        return 1 - 2 * lax.rem(k, 2)

    def far_x(k):
        landed(near.at[pl.ds(0, 2), at(k)], x_in.at[k])
        d = direction(k)
        piece = near.at[lax.rem(x + nx - d, nx), at(k)]
        remote(piece, piece, S_FAR, far_in.at[k], {"x": lax.rem(x + nx + d, nx)}).start()

    def along_z(k):
        landed(near.at[0, at(k)], far_in.at[k])
        d = direction(k)
        target = out.at[at(k), col(z, ylo)]
        remote(near.at[far_z, at(k)], relay.at[at(k)], S_Z, relay_in.at[k],
               {"z": lax.rem(z + nz + d, nz)}).start()
        remote(near.at[up_z, at(k)], target, S_Z, z_in.at[k], {"z": up_z}).start()
        remote(near.at[down_z, at(k)], target, S_Z, z_in.at[k], {"z": down_z}).start()
        pltpu.make_async_copy(near.at[z, at(k)], target, z_in.at[k]).start()

    def relay_z(k):
        landed(relay.at[at(k)], relay_in.at[k])
        d = direction(k)
        source = lax.rem(z + nz - d, nz)
        remote(relay.at[at(k)], out.at[at(k), col(source, ylo)], S_RELAY, z_in.at[k],
               {"z": lax.rem(z + nz + d, nz)}).start()

    def along_y(k):
        landed(out.at[at(k), pl.ds(0, 4 * cols)], z_in.at[k])
        for add in (0, 2):
            piece = out.at[at(k), col(lax.rem(x, 2) + add, ylo)]
            remote(piece, piece, S_Y, y_in.at[k], {"ylo": 1 - ylo}).start()

    def along_x2(k):
        landed(out.at[at(k), pl.ds(0, 2 * cols)], y_in.at[k])
        for add, device in ((0, up_x), (2, down_x)):
            piece = out.at[at(k), col(lax.rem(x, 2) + add, 1 - ylo)]
            remote(piece, piece, S_X2, one.at[R_X2], {"x": device}).start()

    def near_hidden():
        landed(rows_all.at[0, pl.ds(0, 2), 0], one.at[R_HZ])
        for source in (down_z, up_z):
            block = rows_all.at[0, source, c]
            remote(block, block, S_HC, one.at[R_HC], {"c": other}).start()

    def hidden_on(part):
        quarter = own // 4
        for source, device, first in ((down_z, up_z, 0), (up_z, down_z, 2)):
            piece = rows_all.at[0, source, c, pl.ds((first + part) * quarter, quarter)]
            remote(piece, piece, S_HFAR, one.at[R_HFAR], {"z": device}).start()

    def far_hidden():
        landed(rows_all.at[0, 0, 0], one.at[R_HFAR])
        block = rows_all.at[0, far_z, c]
        remote(block, block, S_HC, one.at[R_HC], {"c": other}).start()

    def offset_of(b):
        return lax.rem(b * (7 - b) // 2, 4)

    def hidden_y(j):
        b = j // PIECES
        source = lax.rem(z + offset_of(b), nz)
        lines = pl.ds(pl.multiple_of(lax.rem(j, PIECES) * sub, sub), sub)
        remote(rows_all.at[0, source, c, lines], rows_all.at[1, source, c, lines], S_HY,
               hy_in.at[b], flip).start()

    def hidden_y_in(b):
        block = rows_all.at[1, lax.rem(z + offset_of(b), nz), c]
        landed(block, hy_in.at[b])
        remote(block, block, S_HC2, hc2_in.at[b], {"c": other}).start()

    tile = weight.shape[0] // VOCAB_TILES
    first_id = ((z * 2 + yhi) * 2 + c) * weight.shape[0]

    def dot_step(m, rows, lanes):
        lines = pl.ds(pl.multiple_of(m * tile, tile), tile)
        logits[lines, 0:lanes] = lax.dot_general(
            weight[lines, :], rows.reshape(lanes, hid.shape[1]), (((1,), (1,)), ((), ())),
            preferred_element_type=jnp.float32)

    def stat_step(side, zs, first):
        high = 1 - yhi if side else yhi
        values = logits[:, first:first + LANES]
        top = jnp.max(values, axis=0, keepdims=True)
        total = jnp.sum(jnp.exp(values - top), axis=0, keepdims=True)
        wanted = tokens[side, pl.ds(zs * 2 + high, 1), :] - first_id
        ids = lax.broadcasted_iota(jnp.int32, values.shape, 0)
        hit = jnp.sum(jnp.where(ids == wanted, values, 0.0), axis=0, keepdims=True)
        slot = side * 4 + zs
        stats[slot, 0:1, :] = top
        stats[slot, 1:2, :] = total
        stats[slot, 2:3, :] = hit

    def compute_own(e):
        pair, m = e // (VOCAB_TILES + 1), lax.rem(e, VOCAB_TILES + 1)

        @pl.when(m < VOCAB_TILES)
        def _():
            dot_step(m, rows_all[0, pl.ds(pair * 2, 2)], 2 * LANES)

        @pl.when(m == VOCAB_TILES)
        def _():
            for i in range(2):
                stat_step(0, pair * 2 + i, i * LANES)

    def compute_other(e):
        b, m = e // PERIOD, lax.rem(e, PERIOD)
        zs = lax.rem(z + offset_of(b), nz)

        @pl.when(m == 0)
        def _():
            landed(rows_all.at[1, 0, 0], hc2_in.at[b])

        @pl.when(m < VOCAB_TILES)
        def _():
            dot_step(m, rows_all[1, zs], LANES)

        @pl.when(m == VOCAB_TILES)
        def _():
            stat_step(1, zs, 0)

    events = 2 * (VOCAB_TILES + 1)

    def step(t, carry):
        stages = {"x2": (LAG_X2, along_x2), "y": (LAG_Y, along_y), "relay": (LAG_RELAY, relay_z),
                  "z": (LAG_Z, along_z), "far_x": (LAG_FAR, far_x), "x": (LAG_X, along_x),
                  "swap": (LAG_SWAP, swap), "merge": (0, merge)}
        for lag, stage in (stages[name] for name in ORDER):
            k = t - lag

            @pl.when(jnp.logical_and(k >= 0, k < CHUNKS))
            def _(stage=stage, k=k):
                stage(k)

        pl.when(t == STEP_NEAR)(near_hidden)
        pl.when(t == STEP_ON)(lambda: hidden_on(0))
        pl.when(t == STEP_ON2)(lambda: hidden_on(1))
        pl.when(t == STEP_FAR)(far_hidden)

        piece = t - STEP_HIDDEN

        @pl.when((piece >= EARLY * EVERY) & (lax.rem(piece, EVERY) == 0) & (piece < 4 * PIECES * EVERY))
        def _():
            hidden_y(piece // EVERY)

        block = t - STEP_ARRIVED

        @pl.when((block >= 0) & (lax.rem(block, PERIOD) == 0) & (block < 4 * PERIOD))
        def _():
            hidden_y_in(block // PERIOD)

        @pl.when(t == STEP_OWN)
        def _():
            landed(rows_all.at[0, :, 0], one.at[R_HC])
            landed(weight, one.at[R_WEIGHT])
            landed(tokens.at[1], one.at[R_TOK])

        @pl.when((t >= STEP_OWN) & (t < STEP_OWN + events))
        def _():
            compute_own(t - STEP_OWN)

        @pl.when((t >= STEP_OTHER) & (t < STEP_OTHER + 4 * PERIOD))
        def _():
            compute_other(t - STEP_OTHER)
        return carry

    lax.fori_loop(0, STEPS, step, 0)

    for side in range(2):
        for dz in range(4):
            for dc in range(2):
                zs = lax.rem(z + dz, nz)
                src = stats.at[side * 4 + zs]
                dst = got.at[(side * 4 + z) * 2 + c]
                if side == 0 and dz == 0 and dc == 0:
                    pltpu.make_async_copy(src, dst, one.at[R_STAT]).start()
                else:
                    peer = {"z": zs, "c": lax.rem(c + dc, 2)}
                    remote(src, dst, S_STAT, one.at[R_STAT], peer if side == 0 else {**peer, **flip}).start()
    landed(got, one.at[R_STAT])
    tops = got[:, 0, :]
    top = jnp.max(tops, axis=0, keepdims=True)
    total = jnp.sum(got[:, 1, :] * jnp.exp(tops - top), axis=0, keepdims=True)
    target = jnp.sum(got[:, 2, :], axis=0, keepdims=True)
    logprob[...] = target - top - jnp.log(total)

    landed(out.at[:, pl.ds(0, 2 * cols)], one.at[R_X2])
    landed(halves.at[0], send.at[S_HALF])
    pl.when(swaps)(lambda: landed(merged, send.at[S_SWAP]))
    landed(near.at[pl.ds(0, 2)], send.at[S_X])
    landed(near.at[0], send.at[S_FAR])
    landed(near.at[pl.ds(0, 3)], send.at[S_Z])
    landed(relay, send.at[S_RELAY])
    landed(near.at[pl.ds(0, 2)], send.at[S_Y])
    landed(near.at[pl.ds(0, 2)], send.at[S_X2])
    landed(rows_all.at[0, pl.ds(0, 2), 0], send.at[S_HZ])
    landed(rows_all.at[0, 0, 0], send.at[S_HFAR])
    landed(rows_all.at[0, :, 0], send.at[S_HC])
    landed(rows_all.at[0, :, 0], send.at[S_HY])
    landed(rows_all.at[0, :, 0], send.at[S_HC2])
    landed(tokens.at[0], send.at[S_TOK])
    landed(got.at[pl.ds(0, 15)], send.at[S_STAT])


def write_out(held, both, out, both_out, sem):
    part = held.shape[0] // WRITES
    copies = [pltpu.make_async_copy(held.at[pl.ds(i * part, part)], out.at[pl.ds(i * part, part)], sem.at[i])
              for i in range(WRITES)]
    for copy in copies:
        copy.start()
    values = both[...]
    mine = jnp.where(lax.axis_index("c") == 0, values, pltpu.roll(values, LANES // 2, 1))
    both_out[...] = mine[:, : LANES // 2]
    for copy in copies:
        copy.wait()


def on_device(hidden, tokens, old_weight, new_weight):
    own, width = hidden.shape
    vocab_rows = old_weight.shape[0]
    cols = 2 * new_weight.shape[1]
    sems = pltpu.SemaphoreType.DMA
    engine_weight, both = pl.pallas_call(
        kernel,
        out_shape=(
            pltpu.VMEM((vocab_rows, width), jnp.bfloat16),
            jax.ShapeDtypeStruct((1, LANES), jnp.float32),
        ),
        in_specs=[pl.BlockSpec(memory_space=pltpu.HBM)] * 4,
        out_specs=(pl.BlockSpec(memory_space=pltpu.VMEM), pl.BlockSpec(memory_space=pltpu.VMEM)),
        scratch_shapes=[
            pltpu.VMEM((2, cols // 2, vocab_rows), jnp.bfloat16),
            pltpu.VMEM((vocab_rows, cols), jnp.bfloat16),
            pltpu.VMEM((4, vocab_rows, cols), jnp.bfloat16),
            pltpu.VMEM((vocab_rows, cols), jnp.bfloat16),
            pltpu.VMEM((2, 4, 2, own, width), jnp.bfloat16),
            pltpu.VMEM((vocab_rows, width), jnp.bfloat16),
            pltpu.VMEM((vocab_rows, 4 * own), jnp.float32),
            pltpu.VMEM((8, 8, LANES), jnp.float32),
            pltpu.VMEM((16, 8, LANES), jnp.float32),
            pltpu.VMEM((2, 8, LANES), jnp.int32),
            sems((N_SEND,)),
            sems((N_ONE,)),
            sems((HALVES,)),
            sems((CHUNKS,)),
            sems((CHUNKS,)),
            sems((CHUNKS,)),
            sems((CHUNKS,)),
            sems((CHUNKS,)),
            sems((CHUNKS,)),
            sems((4,)),
            sems((4,)),
        ],
        compiler_params=pltpu.CompilerParams(
            collective_id=0, has_side_effects=True, vmem_limit_bytes=40 * 2**20
        ),
    )(*(pltpu.with_memory_space_constraint(a, pltpu.HBM) for a in (hidden, tokens.reshape(8, LANES), old_weight, new_weight.T)))
    engine_weight, logprob = pl.pallas_call(
        write_out,
        out_shape=(
            jax.ShapeDtypeStruct((vocab_rows, width), jnp.bfloat16),
            jax.ShapeDtypeStruct((1, own), jnp.float32),
        ),
        in_specs=[pl.BlockSpec(memory_space=pl.ANY), pl.BlockSpec(memory_space=pltpu.VMEM)],
        out_specs=(pl.BlockSpec(memory_space=pl.ANY), pl.BlockSpec(memory_space=pltpu.VMEM)),
        scratch_shapes=[sems((WRITES,))],
        compiler_params=pltpu.CompilerParams(vmem_limit_bytes=2**20),
    )(engine_weight, both)
    return logprob.reshape(own), engine_weight


def solution(mesh):
    finer = Mesh(mesh.devices.reshape(4, 2, 4, 2, 2), AXES)
    return jax.shard_map(
        on_device,
        mesh=finer,
        in_specs=(P(DP + VOCAB, None), P(DP), P(VOCAB, None), P(DP, VOCAB)),
        out_specs=(P(DP + VOCAB), P(VOCAB, None)),
        check_vma=False,
    )
```
